32 devices in a mesh: group: 8 (over z, x), tensor: 4 (over y, core).
Axes of the slice: x: 2, y: 2, z: 4, core: 2. Of those that a mesh axis runs over, the one named last changes fastest.
Arguments:
- queries: bfloat16 [1024, 4096], P('group', 'tensor'), may hold values from -120 to 120
- keys: bfloat16 [1024, 512], P('group', 'tensor'), may hold values from -6 to 6
- values: bfloat16 [1024, 512], P('group', 'tensor'), may hold values from -6 to 6
- document_index: int32 [8, 128], P('group'), may hold values from 0 to 7, never falling along the last dimension, each value on 1 to 64 neighbouring positions
- out_proj: bfloat16 [4096, 4096], P('tensor', 'group'), may hold values from -0.25 to 0.25
- residual_in: bfloat16 [1024, 4096], P(('group', 'tensor')), may hold values from -60 to 60
- norm_gain: float32 [4096], replicated, may hold values from 0.1 to 1.9
- expert_ids: int32 [1024, 8], P(('group', 'tensor')), may hold values from 0 to 31, all different within a row; in each aligned block of 32 rows (0 to 31, 32 to 63, ...) at most 16 rows name the same one
- gate_weights: float32 [1024, 8], P(('group', 'tensor')), may hold values from 0.05 to 0.45
- w_gate_up: bfloat16 [32, 4096, 1536], P(('group', 'tensor')), may hold values from -0.09375 to 0.09375
- w_down: bfloat16 [32, 768, 4096], P(('group', 'tensor')), may hold values from -0.21875 to 0.21875
Outputs:
- layer_out: bfloat16 [1024, 4096], P(('group', 'tensor'))
The draws below stay inside these ranges and needn't reach their ends.
Inputs may be any that keep to these rules, and one draw needn't show every extreme that they name: `document_index`: ids never fall along a group's tokens; equal ids mark one document. `expert_ids`: a token names 8 different experts; among the 32 tokens of one device (aligned blocks of rows) no expert is named more than 16 times, a bound that some block reaches.
All inputs are finite; a program needn't handle non-finite values.
Results may differ from the reference program's by a relative error of at most 0.0045.
Values may be sent and summed in bfloat16 or wider, within the bound.
A program may use at most 128 MiB of HBM per device.

```python
import math
import jax
import jax.numpy as jnp
import numpy as np
from jax import lax

D = 4096
QUERY_HEADS = 32
KEY_VALUE_HEADS = 4
HEAD_SIZE = 128
FF = 768
TOPK = 8
TOK_DEV = 32
GROUP_TOKENS = 128
TOTAL_TOKENS = 1024
EXPERTS = 32
CAP = 16
DOCS = 8
N_GROUP = 8


def draw_queries(key, part):
    final_output = jnp.clip(jax.random.normal(jax.random.fold_in(key, 1), (TOTAL_TOKENS, QUERY_HEADS * HEAD_SIZE), jnp.float32), -6.0, 6.0)
    return final_output.astype(jnp.bfloat16)


def draw_keys(key, part):
    final_output = jnp.clip(jax.random.normal(jax.random.fold_in(key, 2), (TOTAL_TOKENS, KEY_VALUE_HEADS * HEAD_SIZE), jnp.float32), -6.0, 6.0)
    return final_output.astype(jnp.bfloat16)


def draw_residual_in(key, part):
    row_scale = jnp.exp(jax.random.uniform(jax.random.fold_in(key, 11), (TOTAL_TOKENS, 1), jnp.float32, jnp.log(0.3), jnp.log(3.0)))
    column_scale = jnp.exp(jax.random.uniform(jax.random.fold_in(key, 12), (1, D), jnp.float32, jnp.log(0.3), jnp.log(3.0)))
    drawn_result = jnp.clip(jax.random.normal(jax.random.fold_in(key, 13), (TOTAL_TOKENS, D), jnp.float32), -6.0, 6.0)
    final_output = drawn_result * row_scale * column_scale
    return final_output.astype(jnp.bfloat16)


def block_scale(own_key, extent, split, low, largest):
    loudness = 1.0
    for dim, parts in split:
        draws = jax.random.uniform(jax.random.fold_in(jax.random.fold_in(own_key, 6), dim), (parts,), jnp.float32, low / len(split), largest / len(split))
        loudness = loudness * jnp.repeat(jnp.exp(draws), extent[dim] // parts).reshape((-1,) + (1,) * (len(extent) - 1 - dim))
    return loudness


def length_profile(number_of, total, limit, skew):
    portions = [(1 << 20) // math.isqrt(grade ** skew) + 1 for grade in range(2, number_of + 1)]
    surplus, given = total - limit - (number_of - 1), [1] * (number_of - 1)
    while surplus > 0:
        movable = [i for i in range(number_of - 1) if given[i] < limit]
        mass, remaining = sum([portions[i] for i in movable]), surplus
        for i in movable:
            more = min(limit - given[i], max(1, remaining * portions[i] // mass), surplus)
            given[i] = given[i] + more
            surplus = surplus - more
    return np.array([limit] + given)


def ragged_sizes(rng, number_of, total, bound, lean):
    if number_of == 2:
        one = jax.random.randint(rng, (), max(1, total - bound), min(bound, total - 1) + 1)
        return jnp.stack([one, total - one])
    sizes = jnp.asarray(length_profile(number_of, total, bound, lean), jnp.int32)
    couples = (number_of - 1) // 2
    donor, receiver = sizes[1:1 + 2 * couples:2], sizes[2:2 + 2 * couples:2]
    slack = jnp.minimum(donor - 1, bound - receiver)
    passed = jax.random.randint(jax.random.fold_in(rng, 1), (couples,), 0, 1 << 20) % (slack + 1)
    sizes = sizes.at[1:1 + 2 * couples:2].set(donor - passed).at[2:2 + 2 * couples:2].set(receiver + passed)
    return sizes[jax.random.permutation(jax.random.fold_in(rng, 2), number_of)]


def shared_out(own_key, own, number, rows, number_of, top, limit, slope):
    sequence = jax.random.permutation(own_key, number_of)
    packed, usual = shares(number_of, rows * top, limit, slope, True), shares(number_of, rows * top, limit, slope, False)
    places = jnp.arange(number_of)

    def named(tallies, offset_by):
        used = int((tallies > 0).sum())
        fixed = max(1, used // 4)
        passed = fixed + (places - fixed + offset_by * (used - fixed)) % max(1, number_of - fixed)
        return jnp.zeros((number_of,), jnp.int32).at[sequence[jnp.where(places < fixed, places, passed)]].set(jnp.asarray(tallies, jnp.int32))

    tallies = jnp.where(number % 4 == 0, named(packed, number // 4), named(usual, number - number // 4 - 1))
    mixed = jax.random.permutation(jax.random.fold_in(own, 3), number_of)
    donor, receiver = mixed[0:number_of // 2 * 2:2], mixed[1:number_of // 2 * 2:2]
    room = jnp.minimum(tallies[donor] - 1, limit - tallies[receiver]) // 2
    room = jnp.where((donor == sequence[0]) | (receiver == sequence[0]) | (tallies[receiver] == 0), 0, jnp.maximum(room, 0))
    passed = jax.random.randint(jax.random.fold_in(own, 4), (number_of // 2,), 0, 1 << 20) % (room + 1)
    tallies = tallies.at[donor].add(-passed).at[receiver].add(passed)
    items = jnp.searchsorted(jnp.cumsum(tallies), jnp.arange(rows * top), side="right").astype(jnp.int32)
    table = items.reshape(top, rows).T
    table = table[jax.random.permutation(jax.random.fold_in(own, 1), rows)]
    offset_by = jax.random.randint(jax.random.fold_in(own, 2), (rows, 1), 0, top)
    return jnp.take_along_axis(table, (jnp.arange(top)[None, :] + offset_by) % top, axis=1)


def shares(amount, total, limit, lean, full):
    portions = [(1 << 20) // math.isqrt(grade ** lean) + 1 for grade in range(1, amount + 1)]
    largest = limit if full else min(limit, max(-(-total // amount), total * portions[0] // sum(portions)))
    least = 1 if total - largest >= amount - 1 else 0
    counts, rest = [largest] + [least] * (amount - 1), total - largest - least * (amount - 1)
    while rest > 0:
        candidates = [i for i in range(1, amount) if counts[i] < largest] or [i for i in range(1, amount) if counts[i] < limit]
        whole, budget = sum([portions[i] for i in candidates]), rest
        for i in candidates:
            extra = min(limit - counts[i], max(1, budget * portions[i] // whole), rest)
            counts[i] = counts[i] + extra
            rest = rest - extra
    return np.array(counts)


def scatter_about(rng, shape, width, reach, shards=(), kind=jnp.bfloat16):
    entries = width * jax.random.normal(rng, shape, jnp.float32)
    if shards:
        entries = entries * block_scale(rng, shape, shards, -0.22, 0.18)
    return jnp.clip(entries, -reach, reach).astype(kind)


def setup_inputs(seed: int = 0) -> dict:
    streams_of = jax.random.split(jax.random.key(seed), 12)
    queries = draw_queries(jax.random.fold_in(streams_of[11], 71), 0)
    keys = draw_keys(jax.random.fold_in(streams_of[11], 71), 0)
    values = scatter_about(streams_of[2], (TOTAL_TOKENS, KEY_VALUE_HEADS * HEAD_SIZE), 1.0, 6.0, ((0, 8), (1, 4)))
    document_index = jax.vmap(lambda own: jnp.searchsorted(jnp.cumsum(ragged_sizes(own, DOCS, GROUP_TOKENS, GROUP_TOKENS // 2, 2)), jnp.arange(GROUP_TOKENS), side="right"))(jax.random.split(streams_of[3], N_GROUP)).reshape((N_GROUP, GROUP_TOKENS)).astype(jnp.int32)
    out_proj = scatter_about(streams_of[4], (QUERY_HEADS * HEAD_SIZE, D), (QUERY_HEADS * HEAD_SIZE // 8) ** -0.5, 0.25, ((0, 4), (1, 8)))
    residual_in = draw_residual_in(jax.random.fold_in(streams_of[11], 71), 0)
    norm_gain = jnp.clip(1.0 + 0.18 * jax.random.normal(streams_of[6], (D,), jnp.float32), 0.1, 1.9)
    expert_ids_keys = jax.random.split(jax.random.fold_in(streams_of[7], 1), TOTAL_TOKENS // TOK_DEV)
    expert_ids_turns = jax.random.permutation(jax.random.fold_in(streams_of[7], 3), TOTAL_TOKENS // TOK_DEV)
    expert_ids = jax.vmap(lambda own, number: shared_out(jax.random.fold_in(streams_of[7], 2), own, number, TOK_DEV, EXPERTS, TOPK, CAP, 2))(expert_ids_keys, expert_ids_turns).reshape((TOTAL_TOKENS, TOPK))
    gate_weights = jnp.clip(0.05 + 0.39999999 * jax.random.uniform(streams_of[8], (TOTAL_TOKENS, TOPK), jnp.float32) ** block_scale(streams_of[8], (TOTAL_TOKENS, TOPK), ((0, 32),), -0.2, 0.2), 0.05, 0.45)
    w_gate_up = scatter_about(streams_of[9], (EXPERTS, D, 2 * FF), D ** -0.5, 0.09375, ((0, 32),))
    w_down = scatter_about(streams_of[10], (EXPERTS, FF, D), FF ** -0.5, 0.21875, ((0, 32),))
    return dict(queries=queries, keys=keys, values=values, document_index=document_index, out_proj=out_proj, residual_in=residual_in, norm_gain=norm_gain, expert_ids=expert_ids, gate_weights=gate_weights, w_gate_up=w_gate_up, w_down=w_down)


def attend(query_matrix, key_matrix, value_matrix, doc_row):
    token_group = query_matrix.shape[0]
    query_head_split = query_matrix.reshape(token_group, KEY_VALUE_HEADS, QUERY_HEADS // KEY_VALUE_HEADS, HEAD_SIZE).astype(jnp.float32)
    key_head_split = key_matrix.reshape(token_group, KEY_VALUE_HEADS, HEAD_SIZE).astype(jnp.float32)
    value_head_split = value_matrix.reshape(token_group, KEY_VALUE_HEADS, HEAD_SIZE).astype(jnp.float32)
    scores = jnp.einsum('qgrd,kgd->grqk', query_head_split, key_head_split) * (1.0 / HEAD_SIZE ** 0.5)
    positions = jnp.arange(token_group, dtype=jnp.int32)
    visible = (positions[:, None] >= positions[None, :]) & (doc_row[:, None] == doc_row[None, :])
    scores = jnp.where(visible, scores, -jnp.inf)
    row_max = lax.optimization_barrier(jnp.max(scores, axis=-1, keepdims=True))
    exponent = jnp.where(visible, jnp.exp(scores - row_max), 0.0)
    weights = (exponent / lax.optimization_barrier(jnp.sum(exponent, axis=-1, keepdims=True))).astype(jnp.bfloat16)
    head_out = jnp.einsum('grqk,kgd->qgrd', weights.astype(jnp.float32), value_head_split)
    return head_out.astype(jnp.bfloat16).reshape(token_group, QUERY_HEADS * HEAD_SIZE)

def reference(queries, keys, values, document_index, out_proj, residual_in, norm_gain, expert_ids, gate_weights, w_gate_up, w_down):
    head_grouped = (queries.reshape(N_GROUP, GROUP_TOKENS, QUERY_HEADS * HEAD_SIZE), keys.reshape(N_GROUP, GROUP_TOKENS, KEY_VALUE_HEADS * HEAD_SIZE), values.reshape(N_GROUP, GROUP_TOKENS, KEY_VALUE_HEADS * HEAD_SIZE), document_index)

    def per_group(inputs):
        return attend(inputs[0], inputs[1], inputs[2], inputs[3])
    head_out = lax.map(per_group, head_grouped).reshape(TOTAL_TOKENS, QUERY_HEADS * HEAD_SIZE)
    hidden = residual_in.astype(jnp.float32) + jnp.dot(head_out, out_proj, preferred_element_type=jnp.float32)
    mean_square = lax.optimization_barrier(jnp.mean(hidden * hidden, axis=-1, keepdims=True))
    normed = (hidden * lax.rsqrt(mean_square + 1e-06) * norm_gain.astype(jnp.float32)).astype(jnp.bfloat16)
    flat_ids = expert_ids.reshape(-1).astype(jnp.int32)
    flat_gate = gate_weights.reshape(-1).astype(jnp.float32)
    token_index = (jnp.arange(TOTAL_TOKENS * TOPK, dtype=jnp.int32) // TOPK).astype(jnp.int32)
    slot_rows = EXPERTS * CAP

    def per_expert(moe_total, inputs):
        expert, gate_up, down_rows = inputs
        chosen = flat_ids == expert
        position = jnp.cumsum(chosen.astype(jnp.int32)) - 1
        position = jnp.where(chosen, position, slot_rows).astype(jnp.int32)
        sources = jnp.zeros((slot_rows,), jnp.int32).at[position].set(token_index, mode='drop')
        weight = jnp.zeros((slot_rows,), jnp.float32).at[position].set(flat_gate, mode='drop')
        gathered_rows = normed[sources]
        projected = jnp.dot(gathered_rows, gate_up, preferred_element_type=jnp.float32)
        activated = (jax.nn.silu(projected[:, :FF]) * projected[:, FF:]).astype(jnp.bfloat16)
        expert_out = jnp.dot(activated, down_rows, preferred_element_type=jnp.float32).astype(jnp.bfloat16)
        moe_total = moe_total.at[sources].add(expert_out.astype(jnp.float32) * weight[:, None])
        return (moe_total, None)
    moe_total, _ = lax.scan(per_expert, jnp.zeros((TOTAL_TOKENS, D), jnp.float32), (jnp.arange(EXPERTS, dtype=jnp.int32), w_gate_up, w_down))
    return (hidden + moe_total).astype(jnp.bfloat16)
```

```python
import functools

import jax
import jax.numpy as jnp
from jax import lax
from jax.experimental import pallas as pl
from jax.experimental.pallas import tpu as pltpu
from jax.sharding import PartitionSpec as P

HEAD_SIZE = 128
LANES = 128


def attention(queries, keys, values, document_index):
    token_group = queries.shape[0]
    kv_dev = keys.shape[1] // HEAD_SIZE
    query_dev = queries.shape[1] // HEAD_SIZE
    group_ratio = query_dev // kv_dev
    query_head_split = queries.reshape(token_group, kv_dev, group_ratio, HEAD_SIZE)
    key_head_split = keys.reshape(token_group, kv_dev, HEAD_SIZE)
    value_head_split = values.reshape(token_group, kv_dev, HEAD_SIZE)
    scores = jnp.einsum(
        "qgrd,kgd->grqk", query_head_split, key_head_split, preferred_element_type=jnp.float32
    ) * (1.0 / HEAD_SIZE**0.5)
    doc_row = document_index[0]
    positions = jnp.arange(token_group, dtype=jnp.int32)
    visible = (positions[:, None] >= positions[None, :]) & (doc_row[:, None] == doc_row[None, :])
    scores = jnp.where(visible, scores, -jnp.inf)
    row_max = jnp.max(scores, axis=-1, keepdims=True)
    exponent = jnp.where(visible, jnp.exp(scores - row_max), 0.0)
    weights = (exponent / jnp.sum(exponent, axis=-1, keepdims=True)).astype(jnp.bfloat16)
    head_out = jnp.einsum(
        "grqk,kgd->qgrd", weights, value_head_split, preferred_element_type=jnp.float32
    )
    return head_out.astype(jnp.bfloat16).reshape(token_group, query_dev * HEAD_SIZE)


MESH = pl.DeviceIdType.MESH
VMEM_LIMIT = 60 * 1024 * 1024


def place(sizes):
    g, t = lax.axis_index("group"), lax.axis_index("tensor")
    return g // 2, g % 2, t // 2, t % 2


def device(z, x, y, c):
    return (z * 2 + x, y * 2 + c)


def enter(partners):
    barrier = pltpu.get_barrier_semaphore()
    for partner in partners:
        pl.semaphore_signal(barrier, inc=1, device_id=partner, device_id_type=MESH)
    pl.semaphore_wait(barrier, len(partners))


def remote(src, dst, send, recv, target):
    return pltpu.make_async_remote_copy(
        src_ref=src,
        dst_ref=dst,
        send_sem=send,
        recv_sem=recv,
        device_id=target,
        device_id_type=MESH,
    )


def project_kernel(
    slabs,
    head_ref,
    w_ref,
    out_ref,
    heads,
    part,
    got_core,
    sum_core,
    got_y,
    sum_y,
    landed,
    z_send,
    z_recv,
    x_send,
    x_recv,
    c_send,
    c_recv,
    y_send,
    y_recv,
    o_send,
    o_recv,
):
    z, x, y, c = place(None)
    width = w_ref.shape[1]
    tok = out_ref.shape[0]
    after = [lax.rem(z + j, slabs) for j in range(slabs)]
    before = [lax.rem(z + slabs - j, slabs) for j in range(slabs)]
    core, over_y, over_x = device(z, x, y, 1 - c), device(z, x, 1 - y, c), device(z, 1 - x, y, c)
    enter(
        [core, over_y]
        + [device(after[j], x, y, c) for j in range(1, slabs)]
        + [device(after[j], 1 - x, y, c) for j in range(slabs)]
    )
    pending = []

    def start(copy):
        copy.start()
        pending.append(copy)
        return copy

    z_copy = [None] * slabs
    x_copy = [None] * slabs
    x_copy[0] = start(remote(head_ref, heads.at[0, 1], x_send.at[0], x_recv.at[0], over_x))
    for j in range(1, slabs):
        z_copy[j] = start(
            remote(
                head_ref, heads.at[j, 0], z_send.at[j], z_recv.at[j], device(before[j], x, y, c)
            )
        )
    c_copy, y_copy, o_copy = [None] * slabs, [None] * slabs, []

    def project(j):
        for side in range(2):
            rows = head_ref if j == 0 and side == 0 else heads.at[j, side]
            got = jnp.dot(rows[...], w_ref[...], preferred_element_type=jnp.float32)
            part[j, :, side] = got.reshape(2, 2, tok, width).transpose(1, 0, 2, 3)
        c_copy[j] = start(
            remote(part.at[j, 1 - c], got_core.at[j], c_send.at[j], c_recv.at[j], core)
        )

    def over_cores(j):
        c_copy[j].wait_recv()
        for side in range(2):
            for row in range(2):
                sum_core[j, row, side] = part[j, c, side, row] + got_core[j, side, row]
        y_copy[j] = start(
            remote(sum_core.at[j, 1 - y], got_y.at[j], y_send.at[j], y_recv.at[j], over_y)
        )

    def over_rows(j):
        y_copy[j].wait_recv()
        for side in range(2):
            total = (sum_core[j, y, side] + got_y[j, side]).astype(jnp.bfloat16)
            if j == 0 and side == 0:
                landed[0, 0] = total
                continue
            sum_y[j, side] = total
            target = device(after[j], x if side == 0 else 1 - x, y, c)
            o_copy.append(
                start(
                    remote(
                        sum_y.at[j, side],
                        landed.at[j, side],
                        o_send.at[j, side],
                        o_recv.at[j, side],
                        target,
                    )
                )
            )

    for j in range(slabs):
        if j + 1 < slabs:
            z_copy[j + 1].wait_recv()
            x_copy[j + 1] = start(
                remote(
                    heads.at[j + 1, 0],
                    heads.at[j + 1, 1],
                    x_send.at[j + 1],
                    x_recv.at[j + 1],
                    over_x,
                )
            )
        x_copy[j].wait_recv()
        project(j)
        if j >= 1:
            over_cores(j - 1)
        if j >= 2:
            over_rows(j - 2)
    over_cores(slabs - 1)
    for j in range(max(slabs - 2, 0), slabs):
        over_rows(j)
    for copy in o_copy:
        copy.wait_recv()
    for copy in pending:
        copy.wait_send()
    for j in range(slabs):
        for side in range(2):
            owner = before[j] * 2 + (x if side == 0 else 1 - x)
            columns = pl.ds(pl.multiple_of(owner * width, width), width)
            out_ref[:, columns] = landed[j, side].astype(jnp.float32)


def project(head_out, out_proj, groups, tok_dev):
    slabs = groups // 2
    tokens, depth = head_out.shape
    width = out_proj.shape[1]
    dma = pltpu.SemaphoreType.DMA
    return pl.pallas_call(
        functools.partial(project_kernel, slabs),
        out_shape=jax.ShapeDtypeStruct((tok_dev, groups * width), jnp.float32),
        in_specs=[pl.BlockSpec(memory_space=pltpu.VMEM)] * 2,
        out_specs=pl.BlockSpec(memory_space=pltpu.VMEM),
        scratch_shapes=[
            pltpu.VMEM((slabs, 2, tokens, depth), jnp.bfloat16),
            pltpu.VMEM((slabs, 2, 2, 2, tok_dev, width), jnp.float32),
            pltpu.VMEM((slabs, 2, 2, tok_dev, width), jnp.float32),
            pltpu.VMEM((slabs, 2, 2, tok_dev, width), jnp.float32),
            pltpu.VMEM((slabs, 2, tok_dev, width), jnp.float32),
            pltpu.VMEM((slabs, 2, tok_dev, width), jnp.bfloat16),
            pltpu.VMEM((slabs, 2, tok_dev, width), jnp.bfloat16),
        ]
        + [dma((slabs,))] * 8
        + [dma((slabs, 2))] * 2,
        compiler_params=pltpu.CompilerParams(
            collective_id=0, has_side_effects=True, vmem_limit_bytes=VMEM_LIMIT
        ),
    )(head_out, out_proj)


def combine_kernel(
    slabs,
    w_ref,
    hidden_ref,
    out_ref,
    got_core,
    sum_core,
    got_a,
    got_b,
    sum_a,
    sum_b,
    last_a,
    last_b,
    done,
    landed,
    c_send,
    c_recv,
    a_send,
    a_recv,
    b_send,
    b_recv,
    la_send,
    la_recv,
    lb_send,
    lb_recv,
    z_send,
    z_recv,
):
    z, x, y, c = place(None)
    tok, width = out_ref.shape
    half = width // 2
    step = 512
    after = [lax.rem(z + j, slabs) for j in range(slabs)]
    core, over_y, over_x = device(z, x, y, 1 - c), device(z, x, 1 - y, c), device(z, 1 - x, y, c)
    enter([core, over_y, over_x] + [device(after[j], x, y, c) for j in range(1, slabs)])
    pending = []

    def start(copy):
        copy.start()
        pending.append(copy)
        return copy

    order = [j for j in range(1, slabs)] + [0]
    c_copy = {
        j: start(
            remote(
                w_ref.at[after[j], :, :, 1 - c],
                got_core.at[j],
                c_send.at[j],
                c_recv.at[j],
                core,
            )
        )
        for j in order
    }
    a_copy, b_copy, la_copy, lb_copy, z_copy = {}, {}, {}, {}, {}

    def add(n, first, second, store):
        @pl.loop(0, n // step)
        def _(i):
            columns = pl.ds(pl.multiple_of(i * step, step), step)
            store(columns, first(columns).astype(jnp.float32) + second(columns).astype(jnp.float32))

    def over_cores(j):
        c_copy[j].wait_recv()
        for u in range(2):
            for v in range(2):

                def store(columns, value):
                    sum_core[j, u, v, :, columns] = value.astype(jnp.bfloat16)

                add(
                    width,
                    lambda columns: w_ref[after[j], u, v, c, :, columns],
                    lambda columns: got_core[j, u, v, :, columns],
                    store,
                )
        a_copy[j] = start(
            remote(
                sum_core.at[j, 1 - x, :, :, pl.ds(0, half)],
                got_a.at[j],
                a_send.at[j],
                a_recv.at[j],
                over_x,
            )
        )
        b_copy[j] = start(
            remote(
                sum_core.at[j, :, 1 - y, :, pl.ds(half, half)],
                got_b.at[j],
                b_send.at[j],
                b_recv.at[j],
                over_y,
            )
        )

    def second(j):
        a_copy[j].wait_recv()
        b_copy[j].wait_recv()
        for v in range(2):

            def store_a(columns, value):
                sum_a[j, v, :, columns] = value.astype(jnp.bfloat16)

            add(
                half,
                lambda columns: sum_core[j, x, v, :, columns],
                lambda columns: got_a[j, v, :, columns],
                store_a,
            )

            def store_b(columns, value):
                sum_b[j, v, :, columns] = value.astype(jnp.bfloat16)

            add(
                half,
                lambda columns: sum_core[
                    j, v, y, :, pl.ds(pl.multiple_of(columns.start + half, step), step)
                ],
                lambda columns: got_b[j, v, :, columns],
                store_b,
            )
        la_copy[j] = start(
            remote(sum_a.at[j, 1 - y], last_a.at[j], la_send.at[j], la_recv.at[j], over_y)
        )
        lb_copy[j] = start(
            remote(sum_b.at[j, 1 - x], last_b.at[j], lb_send.at[j], lb_recv.at[j], over_x)
        )

    def third(j):
        la_copy[j].wait_recv()
        lb_copy[j].wait_recv()

        def store_a(columns, value):
            done[j, :, columns] = value.astype(jnp.bfloat16)

        add(
            half,
            lambda columns: sum_a[j, y, :, columns],
            lambda columns: last_a[j, :, columns],
            store_a,
        )

        def store_b(columns, value):
            shifted = pl.ds(pl.multiple_of(columns.start + half, step), step)
            done[j, :, shifted] = value.astype(jnp.bfloat16)

        add(
            half,
            lambda columns: sum_b[j, x, :, columns],
            lambda columns: last_b[j, :, columns],
            store_b,
        )
        if j:
            z_copy[j] = start(
                remote(
                    done.at[j],
                    landed.at[j],
                    z_send.at[j],
                    z_recv.at[j],
                    device(after[j], x, y, c),
                )
            )

    for i, j in enumerate(order):
        over_cores(j)
        if i >= 1:
            second(order[i - 1])
        if i >= 2:
            third(order[i - 2])
    second(order[-1])
    for j in order[max(slabs - 2, 0) :]:
        third(j)
    for j in range(1, slabs):
        z_copy[j].wait_recv()
    for copy in pending:
        copy.wait_send()

    @pl.loop(0, width // step)
    def _(i):
        columns = pl.ds(pl.multiple_of(i * step, step), step)
        total = hidden_ref[:, columns] + done[0, :, columns].astype(jnp.float32)
        for j in range(1, slabs):
            total = total + landed[j, :, columns].astype(jnp.float32)
        out_ref[:, columns] = total.astype(jnp.bfloat16)


def combine(weighted, hidden, groups):
    slabs = groups // 2
    tok, width = hidden.shape
    half = width // 2
    dma = pltpu.SemaphoreType.DMA
    bf16 = jnp.bfloat16
    return pl.pallas_call(
        functools.partial(combine_kernel, slabs),
        out_shape=jax.ShapeDtypeStruct((tok, width), bf16),
        in_specs=[pl.BlockSpec(memory_space=pltpu.VMEM)] * 2,
        out_specs=pl.BlockSpec(memory_space=pltpu.VMEM),
        scratch_shapes=[
            pltpu.VMEM((slabs, 2, 2, tok, width), bf16),
            pltpu.VMEM((slabs, 2, 2, tok, width), bf16),
            pltpu.VMEM((slabs, 2, tok, half), bf16),
            pltpu.VMEM((slabs, 2, tok, half), bf16),
            pltpu.VMEM((slabs, 2, tok, half), bf16),
            pltpu.VMEM((slabs, 2, tok, half), bf16),
            pltpu.VMEM((slabs, tok, half), bf16),
            pltpu.VMEM((slabs, tok, half), bf16),
            pltpu.VMEM((slabs, tok, width), bf16),
            pltpu.VMEM((slabs, tok, width), bf16),
        ]
        + [dma((slabs,))] * 12,
        compiler_params=pltpu.CompilerParams(
            collective_id=1, has_side_effects=True, vmem_limit_bytes=VMEM_LIMIT
        ),
    )(weighted.reshape(slabs, 2, 2, 2, tok, width), hidden)


def on_device(
    queries,
    keys,
    values,
    document_index,
    out_proj,
    residual_in,
    norm_gain,
    expert_ids,
    gate_weights,
    w_gate_up,
    w_down,
):
    groups, tensors = lax.axis_size("group"), lax.axis_size("tensor")
    experts = groups * tensors
    tok_dev, model_width = residual_in.shape
    head_out = attention(queries, keys, values, document_index)
    attended = project(head_out, out_proj, groups, tok_dev)
    hidden = residual_in.astype(jnp.float32) + attended
    mean_square = jnp.mean(hidden * hidden, axis=-1, keepdims=True)
    normed = (hidden * lax.rsqrt(mean_square + 1e-06) * norm_gain).astype(jnp.bfloat16)
    gates = jnp.sum(
        jnp.where(
            expert_ids[:, :, None] == jnp.arange(experts, dtype=jnp.int32)[None, None, :],
            gate_weights[:, :, None],
            0.0,
        ),
        axis=1,
    )
    high = lax.reduce_precision(gates, 8, 7)
    low = gates - high
    pad = -(2 * experts) % LANES
    extra = jnp.concatenate(
        [high, low, jnp.zeros((tok_dev, pad), jnp.float32)], axis=1
    ).astype(jnp.bfloat16)
    rows = jnp.concatenate([normed, extra], axis=1)
    rows_all = lax.all_gather(rows, ("group", "tensor"), axis=0, tiled=True)
    me = lax.axis_index("group") * tensors + lax.axis_index("tensor")
    picked = jnp.arange(extra.shape[1], dtype=jnp.int32) % experts == me
    picked = picked & (jnp.arange(extra.shape[1], dtype=jnp.int32) < 2 * experts)
    gate_col = jnp.sum(
        jnp.where(picked[None, :], rows_all[:, model_width:].astype(jnp.float32), 0.0),
        axis=1,
        keepdims=True,
    )
    gate_up = w_gate_up[0]
    down_rows = w_down[0]
    ff_width = down_rows.shape[0]
    projected = jnp.dot(rows_all[:, :model_width], gate_up, preferred_element_type=jnp.float32)
    activated = (jax.nn.silu(projected[:, :ff_width]) * projected[:, ff_width:]).astype(
        jnp.bfloat16
    )
    expert_out = jnp.dot(activated, down_rows, preferred_element_type=jnp.float32)
    weighted = (expert_out * gate_col).astype(jnp.bfloat16)
    if weighted.size * 2 * 4 <= VMEM_LIMIT and tensors == 4:
        return combine(weighted, hidden, groups)
    expert_sum = lax.psum_scatter(weighted, ("group", "tensor"), scatter_dimension=0, tiled=True)
    return (hidden + expert_sum.astype(jnp.float32)).astype(jnp.bfloat16)


def solution(mesh):
    in_specs = (
        P("group", "tensor"),
        P("group", "tensor"),
        P("group", "tensor"),
        P("group", None),
        P("tensor", "group"),
        P(("group", "tensor"), None),
        P(),
        P(("group", "tensor"), None),
        P(("group", "tensor"), None),
        P(("group", "tensor"), None, None),
        P(("group", "tensor"), None, None),
    )
    out_specs = P(("group", "tensor"), None)
    return jax.shard_map(
        on_device, mesh=mesh, in_specs=in_specs, out_specs=out_specs, check_vma=False
    )
```

```python
import functools

import jax
import jax.numpy as jnp
from jax import lax
from jax.experimental import pallas as pl
from jax.experimental.pallas import tpu as pltpu
from jax.sharding import PartitionSpec as P

HEAD_SIZE = 128
LANES = 128


def attention(queries, keys, values, document_index):
    token_group = queries.shape[0]
    kv_dev = keys.shape[1] // HEAD_SIZE
    query_dev = queries.shape[1] // HEAD_SIZE
    group_ratio = query_dev // kv_dev
    query_head_split = queries.reshape(token_group, kv_dev, group_ratio, HEAD_SIZE)
    key_head_split = keys.reshape(token_group, kv_dev, HEAD_SIZE)
    value_head_split = values.reshape(token_group, kv_dev, HEAD_SIZE)
    scores = jnp.einsum(
        "qgrd,kgd->grqk", query_head_split, key_head_split, preferred_element_type=jnp.float32
    ) * (1.0 / HEAD_SIZE**0.5)
    doc_row = document_index[0]
    positions = jnp.arange(token_group, dtype=jnp.int32)
    visible = (positions[:, None] >= positions[None, :]) & (doc_row[:, None] == doc_row[None, :])
    scores = jnp.where(visible, scores, -jnp.inf)
    row_max = jnp.max(scores, axis=-1, keepdims=True)
    exponent = jnp.where(visible, jnp.exp(scores - row_max), 0.0)
    weights = (exponent / jnp.sum(exponent, axis=-1, keepdims=True)).astype(jnp.bfloat16)
    head_out = jnp.einsum(
        "grqk,kgd->qgrd", weights, value_head_split, preferred_element_type=jnp.float32
    )
    return head_out.astype(jnp.bfloat16).reshape(token_group, query_dev * HEAD_SIZE)


MESH = pl.DeviceIdType.MESH
VMEM_LIMIT = 60 * 1024 * 1024


def place(sizes):
    g, t = lax.axis_index("group"), lax.axis_index("tensor")
    return g // 2, g % 2, t // 2, t % 2


def device(z, x, y, c):
    return (z * 2 + x, y * 2 + c)


def enter(partners):
    barrier = pltpu.get_barrier_semaphore()
    for partner in partners:
        pl.semaphore_signal(barrier, inc=1, device_id=partner, device_id_type=MESH)
    pl.semaphore_wait(barrier, len(partners))


def remote(src, dst, send, recv, target):
    return pltpu.make_async_remote_copy(
        src_ref=src,
        dst_ref=dst,
        send_sem=send,
        recv_sem=recv,
        device_id=target,
        device_id_type=MESH,
    )


def project_kernel(
    slabs,
    head_ref,
    w_ref,
    out_ref,
    heads,
    part,
    got_core,
    sum_core,
    got_y,
    sum_y,
    landed,
    z_send,
    z_recv,
    x_send,
    x_recv,
    c_send,
    c_recv,
    y_send,
    y_recv,
    o_send,
    o_recv,
):
    z, x, y, c = place(None)
    width = w_ref.shape[1]
    tok = out_ref.shape[0]
    after = [lax.rem(z + j, slabs) for j in range(slabs)]
    before = [lax.rem(z + slabs - j, slabs) for j in range(slabs)]
    core, over_y, over_x = device(z, x, y, 1 - c), device(z, x, 1 - y, c), device(z, 1 - x, y, c)
    enter(
        [core, over_y]
        + [device(after[j], x, y, c) for j in range(1, slabs)]
        + [device(after[j], 1 - x, y, c) for j in range(slabs)]
    )
    pending = []

    def start(copy):
        copy.start()
        pending.append(copy)
        return copy

    z_copy = [None] * slabs
    x_copy = [None] * slabs
    x_copy[0] = start(remote(head_ref, heads.at[0, 1], x_send.at[0], x_recv.at[0], over_x))
    for j in range(1, slabs):
        z_copy[j] = start(
            remote(
                head_ref, heads.at[j, 0], z_send.at[j], z_recv.at[j], device(before[j], x, y, c)
            )
        )
    c_copy, y_copy, o_copy = [None] * slabs, [None] * slabs, []

    def project(j):
        for side in range(2):
            rows = head_ref if j == 0 and side == 0 else heads.at[j, side]
            got = jnp.dot(rows[...], w_ref[...], preferred_element_type=jnp.float32)
            part[j, :, side] = got.reshape(2, 2, tok, width).transpose(1, 0, 2, 3)
        c_copy[j] = start(
            remote(part.at[j, 1 - c], got_core.at[j], c_send.at[j], c_recv.at[j], core)
        )

    def over_cores(j):
        c_copy[j].wait_recv()
        for side in range(2):
            for row in range(2):
                sum_core[j, row, side] = part[j, c, side, row] + got_core[j, side, row]
        y_copy[j] = start(
            remote(sum_core.at[j, 1 - y], got_y.at[j], y_send.at[j], y_recv.at[j], over_y)
        )

    def over_rows(j):
        y_copy[j].wait_recv()
        for side in range(2):
            total = (sum_core[j, y, side] + got_y[j, side]).astype(jnp.bfloat16)
            if j == 0 and side == 0:
                landed[0, 0] = total
                continue
            sum_y[j, side] = total
            target = device(after[j], x if side == 0 else 1 - x, y, c)
            o_copy.append(
                start(
                    remote(
                        sum_y.at[j, side],
                        landed.at[j, side],
                        o_send.at[j, side],
                        o_recv.at[j, side],
                        target,
                    )
                )
            )

    for j in range(slabs):
        if j + 1 < slabs:
            z_copy[j + 1].wait_recv()
            x_copy[j + 1] = start(
                remote(
                    heads.at[j + 1, 0],
                    heads.at[j + 1, 1],
                    x_send.at[j + 1],
                    x_recv.at[j + 1],
                    over_x,
                )
            )
        x_copy[j].wait_recv()
        project(j)
        if j >= 1:
            over_cores(j - 1)
        if j >= 2:
            over_rows(j - 2)
    over_cores(slabs - 1)
    for j in range(max(slabs - 2, 0), slabs):
        over_rows(j)
    for copy in o_copy:
        copy.wait_recv()
    for copy in pending:
        copy.wait_send()
    for j in range(slabs):
        for side in range(2):
            owner = before[j] * 2 + (x if side == 0 else 1 - x)
            columns = pl.ds(pl.multiple_of(owner * width, width), width)
            out_ref[:, columns] = landed[j, side].astype(jnp.float32)


def project(head_out, out_proj, groups, tok_dev):
    slabs = groups // 2
    tokens, depth = head_out.shape
    width = out_proj.shape[1]
    dma = pltpu.SemaphoreType.DMA
    return pl.pallas_call(
        functools.partial(project_kernel, slabs),
        out_shape=jax.ShapeDtypeStruct((tok_dev, groups * width), jnp.float32),
        in_specs=[pl.BlockSpec(memory_space=pltpu.VMEM)] * 2,
        out_specs=pl.BlockSpec(memory_space=pltpu.VMEM),
        scratch_shapes=[
            pltpu.VMEM((slabs, 2, tokens, depth), jnp.bfloat16),
            pltpu.VMEM((slabs, 2, 2, 2, tok_dev, width), jnp.float32),
            pltpu.VMEM((slabs, 2, 2, tok_dev, width), jnp.float32),
            pltpu.VMEM((slabs, 2, 2, tok_dev, width), jnp.float32),
            pltpu.VMEM((slabs, 2, tok_dev, width), jnp.float32),
            pltpu.VMEM((slabs, 2, tok_dev, width), jnp.bfloat16),
            pltpu.VMEM((slabs, 2, tok_dev, width), jnp.bfloat16),
        ]
        + [dma((slabs,))] * 8
        + [dma((slabs, 2))] * 2,
        compiler_params=pltpu.CompilerParams(
            collective_id=0, has_side_effects=True, vmem_limit_bytes=VMEM_LIMIT
        ),
    )(head_out, out_proj)


def combine_kernel(
    slabs,
    w_ref,
    hidden_ref,
    out_ref,
    got_core,
    sum_core,
    got_a,
    got_b,
    sum_a,
    sum_b,
    last_a,
    last_b,
    done,
    landed,
    c_send,
    c_recv,
    a_send,
    a_recv,
    b_send,
    b_recv,
    la_send,
    la_recv,
    lb_send,
    lb_recv,
    z_send,
    z_recv,
):
    z, x, y, c = place(None)
    tok, width = out_ref.shape
    half = width // 2
    step = 512
    after = [lax.rem(z + j, slabs) for j in range(slabs)]
    core, over_y, over_x = device(z, x, y, 1 - c), device(z, x, 1 - y, c), device(z, 1 - x, y, c)
    enter([core, over_y, over_x] + [device(after[j], x, y, c) for j in range(1, slabs)])
    pending = []

    def start(copy):
        copy.start()
        pending.append(copy)
        return copy

    order = [j for j in range(1, slabs)] + [0]
    c_copy = {
        j: start(
            remote(
                w_ref.at[after[j], :, :, 1 - c],
                got_core.at[j],
                c_send.at[j],
                c_recv.at[j],
                core,
            )
        )
        for j in order
    }
    a_copy, b_copy, la_copy, lb_copy, z_copy = {}, {}, {}, {}, {}

    def add(n, first, second, store):
        @pl.loop(0, n // step)
        def _(i):
            columns = pl.ds(pl.multiple_of(i * step, step), step)
            store(columns, first(columns).astype(jnp.float32) + second(columns).astype(jnp.float32))

    def over_cores(j):
        c_copy[j].wait_recv()
        for u in range(2):
            for v in range(2):

                def store(columns, value):
                    sum_core[j, u, v, :, columns] = value.astype(jnp.bfloat16)

                add(
                    width,
                    lambda columns: w_ref[after[j], u, v, c, :, columns],
                    lambda columns: got_core[j, u, v, :, columns],
                    store,
                )
        a_copy[j] = start(
            remote(
                sum_core.at[j, 1 - x, :, :, pl.ds(0, half)],
                got_a.at[j],
                a_send.at[j],
                a_recv.at[j],
                over_x,
            )
        )
        b_copy[j] = start(
            remote(
                sum_core.at[j, :, 1 - y, :, pl.ds(half, half)],
                got_b.at[j],
                b_send.at[j],
                b_recv.at[j],
                over_y,
            )
        )

    def second(j):
        a_copy[j].wait_recv()
        b_copy[j].wait_recv()
        for v in range(2):

            def store_a(columns, value):
                sum_a[j, v, :, columns] = value.astype(jnp.bfloat16)

            add(
                half,
                lambda columns: sum_core[j, x, v, :, columns],
                lambda columns: got_a[j, v, :, columns],
                store_a,
            )

            def store_b(columns, value):
                sum_b[j, v, :, columns] = value.astype(jnp.bfloat16)

            add(
                half,
                lambda columns: sum_core[
                    j, v, y, :, pl.ds(pl.multiple_of(columns.start + half, step), step)
                ],
                lambda columns: got_b[j, v, :, columns],
                store_b,
            )
        la_copy[j] = start(
            remote(sum_a.at[j, 1 - y], last_a.at[j], la_send.at[j], la_recv.at[j], over_y)
        )
        lb_copy[j] = start(
            remote(sum_b.at[j, 1 - x], last_b.at[j], lb_send.at[j], lb_recv.at[j], over_x)
        )

    def third(j):
        la_copy[j].wait_recv()
        lb_copy[j].wait_recv()

        def store_a(columns, value):
            done[j, :, columns] = value.astype(jnp.bfloat16)

        add(
            half,
            lambda columns: sum_a[j, y, :, columns],
            lambda columns: last_a[j, :, columns],
            store_a,
        )

        def store_b(columns, value):
            shifted = pl.ds(pl.multiple_of(columns.start + half, step), step)
            done[j, :, shifted] = value.astype(jnp.bfloat16)

        add(
            half,
            lambda columns: sum_b[j, x, :, columns],
            lambda columns: last_b[j, :, columns],
            store_b,
        )
        if j:
            z_copy[j] = start(
                remote(
                    done.at[j],
                    landed.at[j],
                    z_send.at[j],
                    z_recv.at[j],
                    device(after[j], x, y, c),
                )
            )

    for i, j in enumerate(order):
        over_cores(j)
        if i >= 1:
            second(order[i - 1])
        if i >= 2:
            third(order[i - 2])
    second(order[-1])
    for j in order[max(slabs - 2, 0) :]:
        third(j)
    for j in range(1, slabs):
        z_copy[j].wait_recv()
    for copy in pending:
        copy.wait_send()

    @pl.loop(0, width // step)
    def _(i):
        columns = pl.ds(pl.multiple_of(i * step, step), step)
        total = hidden_ref[:, columns] + done[0, :, columns].astype(jnp.float32)
        for j in range(1, slabs):
            total = total + landed[j, :, columns].astype(jnp.float32)
        out_ref[:, columns] = total.astype(jnp.bfloat16)


def combine(weighted, hidden, groups):
    slabs = groups // 2
    tok, width = hidden.shape
    half = width // 2
    dma = pltpu.SemaphoreType.DMA
    bf16 = jnp.bfloat16
    return pl.pallas_call(
        functools.partial(combine_kernel, slabs),
        out_shape=jax.ShapeDtypeStruct((tok, width), bf16),
        in_specs=[pl.BlockSpec(memory_space=pltpu.VMEM)] * 2,
        out_specs=pl.BlockSpec(memory_space=pltpu.VMEM),
        scratch_shapes=[
            pltpu.VMEM((slabs, 2, 2, tok, width), bf16),
            pltpu.VMEM((slabs, 2, 2, tok, width), bf16),
            pltpu.VMEM((slabs, 2, tok, half), bf16),
            pltpu.VMEM((slabs, 2, tok, half), bf16),
            pltpu.VMEM((slabs, 2, tok, half), bf16),
            pltpu.VMEM((slabs, 2, tok, half), bf16),
            pltpu.VMEM((slabs, tok, half), bf16),
            pltpu.VMEM((slabs, tok, half), bf16),
            pltpu.VMEM((slabs, tok, width), bf16),
            pltpu.VMEM((slabs, tok, width), bf16),
        ]
        + [dma((slabs,))] * 12,
        compiler_params=pltpu.CompilerParams(
            collective_id=1, has_side_effects=True, vmem_limit_bytes=VMEM_LIMIT
        ),
    )(weighted.reshape(slabs, 2, 2, 2, tok, width), hidden)


def gather_kernel(slabs, half, rows_ref, out_ref, own_sem, *sems):
    z, x, y, c = place(None)
    width = rows_ref.shape[1]
    low, high = pl.ds(0, half), pl.ds(half, width - half)
    after = [lax.rem(z + j, slabs) for j in range(slabs)]
    before = [lax.rem(z + slabs - j, slabs) for j in range(slabs)]
    core, over_y, over_x = device(z, x, y, 1 - c), device(z, x, 1 - y, c), device(z, 1 - x, y, c)
    own = pltpu.make_async_copy(rows_ref, out_ref.at[z, x, y, c], own_sem)
    own.start()
    enter([core, over_y, over_x] + [device(after[j], x, y, c) for j in range(1, slabs)])
    copies = {}

    def send(kind, j, src, dst, target):
        copy = remote(src, dst, sems[2 * kind].at[j], sems[2 * kind + 1].at[j], target)
        copy.start()
        copies[kind, j] = copy

    def pass_on(kind, j, block, target):
        send(kind, j, block, block, target)

    for j in range(1, slabs):
        send(0, j, rows_ref, out_ref.at[z, x, y, c], device(before[j], x, y, c))

    def first(j):
        if j:
            copies[0, j].wait_recv()
        else:
            own.wait()
        pass_on(1, j, out_ref.at[after[j], x, y, c, :, low], over_x)
        pass_on(2, j, out_ref.at[after[j], x, y, c, :, high], over_y)
        pass_on(3, j, out_ref.at[after[j], x, y, c], core)

    def second(j):
        copies[1, j].wait_recv()
        pass_on(4, j, out_ref.at[after[j], :, y, c, :, low], over_y)
        pass_on(5, j, out_ref.at[after[j], 1 - x, y, c, :, low], core)
        copies[2, j].wait_recv()
        pass_on(6, j, out_ref.at[after[j], x, :, c, :, high], over_x)
        pass_on(7, j, out_ref.at[after[j], x, 1 - y, c, :, high], core)

    def third(j):
        copies[4, j].wait_recv()
        pass_on(8, j, out_ref.at[after[j], :, 1 - y, c, :, low], core)
        copies[6, j].wait_recv()
        pass_on(9, j, out_ref.at[after[j], 1 - x, :, c, :, high], core)

    for j in range(slabs + 2):
        if j < slabs:
            first(j)
        if 0 <= j - 1 < slabs:
            second(j - 1)
        if 0 <= j - 2:
            third(j - 2)
    for (kind, _), copy in copies.items():
        if kind in (3, 5, 7, 8, 9):
            copy.wait_recv()
        copy.wait_send()


def gather(rows, groups):
    slabs = groups // 2
    tok, width = rows.shape
    half = width // LANES // 2 * LANES
    dma = pltpu.SemaphoreType.DMA
    out = pl.pallas_call(
        functools.partial(gather_kernel, slabs, half),
        out_shape=jax.ShapeDtypeStruct((slabs, 2, 2, 2, tok, width), rows.dtype),
        in_specs=[pl.BlockSpec(memory_space=pltpu.VMEM)],
        out_specs=pl.BlockSpec(memory_space=pltpu.VMEM),
        scratch_shapes=[dma] + [dma((slabs,))] * 20,
        compiler_params=pltpu.CompilerParams(
            collective_id=2, has_side_effects=True, vmem_limit_bytes=VMEM_LIMIT // 2
        ),
    )(rows)
    return out.reshape(slabs * 8 * tok, width)


def on_device(
    queries,
    keys,
    values,
    document_index,
    out_proj,
    residual_in,
    norm_gain,
    expert_ids,
    gate_weights,
    w_gate_up,
    w_down,
):
    groups, tensors = lax.axis_size("group"), lax.axis_size("tensor")
    experts = groups * tensors
    tok_dev, model_width = residual_in.shape
    head_out = attention(queries, keys, values, document_index)
    attended = project(head_out, out_proj, groups, tok_dev)
    hidden = residual_in.astype(jnp.float32) + attended
    mean_square = jnp.mean(hidden * hidden, axis=-1, keepdims=True)
    normed = (hidden * lax.rsqrt(mean_square + 1e-06) * norm_gain).astype(jnp.bfloat16)
    gates = jnp.sum(
        jnp.where(
            expert_ids[:, :, None] == jnp.arange(experts, dtype=jnp.int32)[None, None, :],
            gate_weights[:, :, None],
            0.0,
        ),
        axis=1,
    )
    high = lax.reduce_precision(gates, 8, 7)
    low = gates - high
    pad = -(2 * experts) % LANES
    extra = jnp.concatenate(
        [high, low, jnp.zeros((tok_dev, pad), jnp.float32)], axis=1
    ).astype(jnp.bfloat16)
    rows = jnp.concatenate([normed, extra], axis=1)
    on_chip = experts * rows.size * 2 * 4 <= VMEM_LIMIT and tensors == 4
    if on_chip:
        rows_all = gather(rows, groups)
    else:
        rows_all = lax.all_gather(rows, ("group", "tensor"), axis=0, tiled=True)
    me = lax.axis_index("group") * tensors + lax.axis_index("tensor")
    picked = jnp.arange(extra.shape[1], dtype=jnp.int32) % experts == me
    picked = picked & (jnp.arange(extra.shape[1], dtype=jnp.int32) < 2 * experts)
    gate_col = jnp.sum(
        jnp.where(picked[None, :], rows_all[:, model_width:].astype(jnp.float32), 0.0),
        axis=1,
        keepdims=True,
    )
    gate_up = w_gate_up[0]
    down_rows = w_down[0]
    ff_width = down_rows.shape[0]
    projected = jnp.dot(rows_all[:, :model_width], gate_up, preferred_element_type=jnp.float32)
    activated = (jax.nn.silu(projected[:, :ff_width]) * projected[:, ff_width:]).astype(
        jnp.bfloat16
    )
    expert_out = jnp.dot(activated, down_rows, preferred_element_type=jnp.float32)
    weighted = (expert_out * gate_col).astype(jnp.bfloat16)
    if on_chip:
        return combine(weighted, hidden, groups)
    expert_sum = lax.psum_scatter(weighted, ("group", "tensor"), scatter_dimension=0, tiled=True)
    return (hidden + expert_sum.astype(jnp.float32)).astype(jnp.bfloat16)


def solution(mesh):
    in_specs = (
        P("group", "tensor"),
        P("group", "tensor"),
        P("group", "tensor"),
        P("group", None),
        P("tensor", "group"),
        P(("group", "tensor"), None),
        P(),
        P(("group", "tensor"), None),
        P(("group", "tensor"), None),
        P(("group", "tensor"), None, None),
        P(("group", "tensor"), None, None),
    )
    out_specs = P(("group", "tensor"), None)
    return jax.shard_map(
        on_device, mesh=mesh, in_specs=in_specs, out_specs=out_specs, check_vma=False
    )
```
